256 devices in a mesh: row: 32 (over y, z), col: 8 (over x, core).
Axes of the slice: x: 4, y: 4, z: 8, core: 2. Of those that a mesh axis runs over, the one named last changes fastest.
Arguments:
- eigvecs: float32 [131072, 1024], P('row', 'col'), may hold values from -6 to 6
- reflectors: float32 [4, 131072, 256], P(None, ('row', 'col'))
- factors: float32 [4, 256, 256], replicated, as said below
Outputs:
- transformed: float32 [131072, 1024], P('row', 'col')
The draws below stay inside these ranges and needn't reach their ends.
Inputs may be any that keep to these rules, and one draw needn't show every extreme that they name: Each factors[k] is upper triangular with a positive diagonal.
All inputs are finite; a program needn't handle non-finite values.
Results may differ from the reference program's by a relative error of at most 0.00012.
Values sent between devices are 32-bit elements; how exact they have to be, the bound alone decides.
No kernel may reach another device: no remote copies, remote signals or barrier semaphores. Data moves between devices by JAX's collectives and lax.ppermute only.
A program may use at most 128 MiB of HBM per device.

```python
import jax
import jax.numpy as jnp
from jax import lax

N = 131072
M = 1024
WB = 256
PANELS = 4


def draw_reflectors(key, part):
    scale = (N * WB) ** (-0.25)
    base = jnp.clip(jax.random.normal(key, (PANELS, N, WB), jnp.float32), -6.0, 6.0)
    return base * scale


def draw_factors(key, part):
    diag = jax.random.uniform(key, (PANELS, WB), jnp.float32, 0.5, 1.5)
    off = 0.5 * jnp.clip(jax.random.normal(jax.random.fold_in(key, 3), (PANELS, WB, WB), jnp.float32), -6.0, 6.0) / jnp.sqrt(WB * 1.0)
    upper = jnp.triu(off, 1)
    eye = jnp.eye(WB, dtype=jnp.float32)
    return upper + eye[None, :, :] * diag[:, None, :]


def block_scale(rng, dims, pieces, low, top_value):
    def one(position, parts):
        heights = jax.random.uniform(jax.random.fold_in(jax.random.fold_in(rng, 6), position), (parts,), jnp.float32, low / len(pieces), top_value / len(pieces))
        return jnp.repeat(jnp.exp(heights), dims[position] // parts).reshape((-1,) + (1,) * (len(dims) - position - 1))

    factor_of = one(*pieces[0])
    for cut in pieces[1:]:
        factor_of = factor_of * one(*cut)
    return factor_of


def scatter_about(stream_key, dims, deviation, reach, split=(), kind=jnp.bfloat16):
    array = deviation * jax.random.normal(stream_key, dims, jnp.float32)
    if split:
        array = array * block_scale(stream_key, dims, split, -0.22, 0.18)
    return jnp.clip(array, -reach, reach).astype(kind)


def setup_inputs(seed: int = 0) -> dict:
    splits = jax.random.split(jax.random.key(seed), 4)
    return {
        "eigvecs": scatter_about(splits[0], (N, M), 1.0, 6.0, ((0, 32), (1, 8)), jnp.float32),
        "reflectors": draw_reflectors(jax.random.fold_in(splits[3], 71), 0),
        "factors": draw_factors(jax.random.fold_in(splits[3], 71), 0),
    }


def reference(eigvecs, reflectors, factors):
    field = eigvecs
    for index in range(PANELS):
        vectors = reflectors[index]
        proj = lax.dot_general(vectors, field, (((0,), (0,)), ((), ())), precision=lax.Precision.HIGHEST, preferred_element_type=jnp.float32)
        coeffs = jnp.dot(factors[index], proj, precision=lax.Precision.HIGHEST, preferred_element_type=jnp.float32)
        field = field - jnp.dot(vectors, coeffs, precision=lax.Precision.HIGHEST, preferred_element_type=jnp.float32)
    return field
```

```python
import jax
import jax.numpy as jnp
from jax import lax
from jax.experimental import pallas as pl
from jax.experimental.pallas import tpu as pltpu
from jax.sharding import Mesh
from jax.sharding import PartitionSpec as P


ROW = ("y", "z")
COL = ("x", "core")
SMEM = pl.BlockSpec(memory_space=pltpu.SMEM)
VMEM = pl.BlockSpec(memory_space=pltpu.VMEM)
ANY = pl.BlockSpec(memory_space=pl.ANY)
F32, BF16 = jnp.float32, jnp.bfloat16
DISTANCES = (0, 3, 1, 2)
ROWS = 512


def dot(left, right):
    return jnp.dot(left, right, preferred_element_type=F32)


def halves(x):
    high = x.astype(BF16)
    return high, (x - high.astype(F32)).astype(BF16)


def product(left, right):
    lh, ll = halves(left)
    rh, rl = halves(right)
    wide = dot(lh, jnp.concatenate([rh, rl], axis=1))
    return wide[:, :128] + wide[:, 128:] + dot(ll, rh)


def starts(place_ref):
    out = []
    for side in range(2):
        for distance in DISTANCES:
            block = lax.rem(place_ref[0] + distance, 4) * 2 + lax.rem(place_ref[1] + side, 2)
            out.append(pl.multiple_of(block * ROWS, ROWS))
    return out


def piece_refs(refs, panel):
    own, swapped = refs[0].at[panel], refs[1].at[panel]
    moved = refs[2 + 6 * (panel % 2) : 8 + 6 * (panel % 2)]
    return [own, *moved[:3], swapped, *moved[3:]]


def fetch(pairs, sems):
    copies = [pltpu.make_async_copy(source, target, sems.at[i]) for i, (source, target) in enumerate(pairs)]
    for copy in copies:
        copy.start()
    return copies


def turned(x):
    high, low = halves(x.T)
    return jnp.concatenate([high, low], axis=0)


def project(left, values, totals, first):
    high, low = halves(values)
    wide, narrow = dot(left, high), dot(left[:128], low)
    part = wide[:128] + wide[128:] + narrow
    totals[...] = part if first else totals[...] + part


def project_kernel(place_ref, e_ref, *refs):
    pieces, (out_ref, field, held, totals, sems) = refs[:-5], refs[-5:]
    where = starts(place_ref)
    pairs = [(e_ref, field)]
    for i in range(8):
        pairs += [(piece_refs(pieces, panel)[i], held.at[panel, i]) for panel in range(2)]
    copies = fetch(pairs, sems)
    copies[0].wait()
    for i in range(8):
        left = turned(field[pl.ds(where[i], ROWS), :])
        for panel in range(2):
            copies[1 + 2 * i + panel].wait()
            project(left, held[panel, i], totals.at[panel], i == 0)
    for panel in range(2):
        out_ref[:, 8 * panel : 8 * panel + 8, :] = totals[panel].T.reshape(32, 8, 128)


def solved(place_ref, sums_ref, factors, mine, other, pair):
    gram = jnp.where(place_ref[1] == pair, mine[...], other[...])
    first = product(factors[0], sums_ref[:, 0:8, :].reshape(256, 128))
    left = sums_ref[:, 8:16, :].reshape(256, 128) - product(gram, first)
    return [halves(first), halves(product(factors[1], left))]


def moved(parts, values):
    total = None
    for (high, low), v in zip(parts, values):
        vh, vl = halves(v)
        wide = dot(vh, jnp.concatenate([high, low], axis=1))
        part = wide[:, :128] + wide[:, 128:] + dot(vl, high)
        total = part if total is None else total + part
    return total


def middle_kernel(place_ref, e_ref, sums_ref, factors_ref, mine_ref, other_ref, *refs):
    early, late = refs[:14], refs[14:26]
    out_ref, tiles_ref, field, new, sums, factors, mine, other, held, later, totals, sems, out_sems = refs[26:]
    where = starts(place_ref)
    late = (*early[:2], *late)
    pairs = [(sums_ref, sums), (factors_ref.at[0:2], factors), (mine_ref, mine), (other_ref, other), (e_ref, field)]
    for i in range(8):
        pairs += [(piece_refs(early, panel)[i], held.at[panel, i]) for panel in range(2)]
        pairs += [(piece_refs(late, 2 + panel)[i], later.at[panel, i]) for panel in range(2)]
    copies = fetch(pairs, sems)
    for copy in copies[:4]:
        copy.wait()
    parts = solved(place_ref, sums, factors, mine, other, 0)
    copies[4].wait()
    outs = []
    for i in range(8):
        rows = pl.ds(where[i], ROWS)
        for copy in copies[5 + 4 * i : 9 + 4 * i]:
            copy.wait()
        value = field[rows, :] - moved(parts, [held[0, i], held[1, i]])
        new[i] = value
        outs.append(pltpu.make_async_copy(new.at[i], out_ref.at[rows, :], out_sems.at[i]))
        outs[-1].start()
        left = turned(value)
        for panel in range(2):
            project(left, later[panel, i], totals.at[panel], i == 0)
    for panel in range(2):
        tiles_ref[:, 8 * panel : 8 * panel + 8, :] = totals[panel].T.reshape(32, 8, 128)
    for copy in outs:
        copy.wait()


def last_kernel(place_ref, field_ref, sums_ref, factors_ref, mine_ref, other_ref, *refs):
    pieces, (out_ref, field, new, sums, factors, mine, other, held, sems, out_sems) = refs[:-10], refs[-10:]
    where = starts(place_ref)
    pairs = [(sums_ref, sums), (factors_ref.at[2:4], factors), (mine_ref, mine), (other_ref, other), (field_ref, field)]
    for i in range(8):
        pairs += [(piece_refs(pieces, 2 + panel)[i], held.at[panel, i]) for panel in range(2)]
    copies = fetch(pairs, sems)
    for copy in copies[:4]:
        copy.wait()
    parts = solved(place_ref, sums, factors, mine, other, 1)
    copies[4].wait()
    outs = []
    for i in range(8):
        rows = pl.ds(where[i], ROWS)
        for copy in copies[5 + 2 * i : 7 + 2 * i]:
            copy.wait()
        new[i] = field[rows, :] - moved(parts, [held[0, i], held[1, i]])
        outs.append(pltpu.make_async_copy(new.at[i], out_ref.at[rows, :], out_sems.at[i]))
        outs[-1].start()
    for copy in outs:
        copy.wait()


def gram_kernel(place_ref, panels_ref, mine_ref, other_ref):
    for pair in range(2):
        lh, ll = halves(panels_ref[2 * pair + 1].T)
        high, low = halves(panels_ref[2 * pair])
        block = dot(lh, high) + dot(lh, low) + dot(ll, high)

        @pl.when(place_ref[1] == pair)
        def _():
            mine_ref[...] = block

        @pl.when(place_ref[1] != pair)
        def _():
            other_ref[...] = block


def spread_kernel(arrived_ref, out_ref):
    total = jnp.sum(arrived_ref[...], axis=0)
    out_ref[...] = jnp.broadcast_to(total[None], out_ref.shape)


def call(kernel, out, ins, outs, scratch, *args):
    return pl.pallas_call(kernel, out_shape=out, in_specs=ins, out_specs=outs, scratch_shapes=scratch,
                          compiler_params=pltpu.CompilerParams(vmem_limit_bytes=40 * 2**20))(*args)


def shifted(x, axis, step):
    size = lax.axis_size(axis)
    return lax.ppermute(x, axis, [(i, (i + step) % size) for i in range(size)])


def gathered(k, own):
    behind = shifted(own, "x", 1)
    ahead = shifted(own, "x", -1)
    far = shifted(*((behind, "x", 1) if k % 2 == 0 else (ahead, "x", -1)))
    mine = [behind, ahead, far]
    return mine + [shifted(part, "core", 1) for part in mine]


def exchanged(tiles):
    return lax.all_to_all(tiles, ROW, split_axis=0, concat_axis=0, tiled=True)


def total(tiles):
    arrived = exchanged(tiles)
    copies = call(spread_kernel, jax.ShapeDtypeStruct(tiles.shape, F32), [VMEM], VMEM, [], arrived)
    return exchanged(copies)


def gram(reflectors, place):
    share = jax.ShapeDtypeStruct((256, 256), F32)
    mine, other = call(gram_kernel, [share, share], [SMEM, VMEM], [VMEM, VMEM], [], place, reflectors)
    mine = mine + shifted(other, "core", 1)
    part = exchanged(mine.reshape(32, 8, 256)).sum(axis=0)
    part = (part + shifted(part, "x", 2)) + (shifted(part, "x", 1) + shifted(part, "x", -1))
    copies = jnp.broadcast_to(lax.optimization_barrier(part), (32, 8, 256))
    mine = exchanged(copies).reshape(256, 256)
    return mine, shifted(mine, "core", 1)


def body(eigvecs, reflectors, factors):
    place = jnp.stack([lax.axis_index("x"), lax.axis_index("core")]).astype(jnp.int32)
    swapped = shifted(reflectors, "core", 1)
    moving = [gathered(k, reflectors[k]) for k in range(4)]
    mine, other = gram(reflectors, place)
    whole, tiles = jax.ShapeDtypeStruct((4096, 128), F32), jax.ShapeDtypeStruct((32, 16, 128), F32)
    early, late = (*moving[0], *moving[1]), (*moving[2], *moving[3])
    sem = pltpu.SemaphoreType.DMA
    field = pltpu.VMEM((4096, 128), F32)
    held, totals = pltpu.VMEM((2, 8, ROWS, 256), F32), pltpu.VMEM((2, 128, 256), F32)
    new, square = pltpu.VMEM((8, ROWS, 128), F32), pltpu.VMEM((256, 256), F32)
    small = [pltpu.VMEM((32, 16, 128), F32), pltpu.VMEM((2, 256, 256), F32), square, square]
    sums = call(project_kernel, tiles, [SMEM] + [ANY] * 15, VMEM, [field, held, totals, sem((17,))],
                place, eigvecs, reflectors, swapped, *early)
    sums = total(sums)
    rest, sums = call(middle_kernel, [whole, tiles], [SMEM] + [ANY] * 31, [ANY, VMEM],
                      [field, new, *small, held, held, totals, sem((37,)), sem((8,))],
                      place, eigvecs, sums, factors, mine, other, reflectors, swapped, *early, *late)
    sums = total(sums)
    return call(last_kernel, whole, [SMEM] + [ANY] * 19, ANY,
                [field, new, *small, held, sem((21,)), sem((8,))],
                place, rest, sums, factors, mine, other, reflectors, swapped, *late)


def solution(mesh):
    split = Mesh(mesh.devices.reshape(4, 8, 4, 2), (*ROW, *COL))
    in_specs = (P(ROW, COL), P(None, ROW + COL, None), P())
    return jax.shard_map(body, mesh=split, in_specs=in_specs, out_specs=P(ROW, COL), check_vma=False)
```

```python
import functools

import jax
import jax.numpy as jnp
from jax import lax
from jax.experimental import pallas as pl
from jax.experimental.pallas import tpu as pltpu
from jax.sharding import Mesh
from jax.sharding import PartitionSpec as P


ROW = ("y", "z")
COL = ("x", "core")
SMEM = pl.BlockSpec(memory_space=pltpu.SMEM)
VMEM = pl.BlockSpec(memory_space=pltpu.VMEM)
ANY = pl.BlockSpec(memory_space=pltpu.HBM)
F32, BF16 = jnp.float32, jnp.bfloat16
DISTANCES = (0, 3, 1, 2)
ROWS = 512
BLOCKS = ((1, 0), (2, 0), (2, 1), (3, 0), (3, 1), (3, 2))


def dot(left, right):
    return jnp.dot(left, right, preferred_element_type=F32)


def halves(x):
    high = x.astype(BF16)
    return high, (x - high.astype(F32)).astype(BF16)


def product(left, right):
    lh, ll = halves(left)
    rh, rl = halves(right)
    wide = dot(lh, jnp.concatenate([rh, rl], axis=1))
    return wide[:, :128] + wide[:, 128:] + dot(ll, rh)


def starts(place_ref):
    out = []
    for side in range(2):
        for distance in DISTANCES:
            block = lax.rem(place_ref[0] + distance, 4) * 2 + lax.rem(place_ref[1] + side, 2)
            out.append(pl.multiple_of(block * ROWS, ROWS))
    return out


def fetch(pairs, sems):
    copies = [pltpu.make_async_copy(source, target, sems.at[i]) for i, (source, target) in enumerate(pairs)]
    for copy in copies:
        copy.start()
    return copies


def panel_of(piece, panel):
    return piece.at[panel if piece.shape[0] == 4 else panel % 2]


def turned(x):
    high, low = halves(x.T)
    return jnp.concatenate([high, low], axis=0)


def crossed(left, high, low):
    wide = dot(left, high)
    return wide[:128] + wide[128:] + dot(left[:128], low)


def stage_kernel(items, first, last, place_ref, e_ref, *refs):
    olds, refs = (refs[:0], refs) if first else (refs[:1], refs[1:])
    pieces, (out_ref, field, held, sums, sems) = refs[: len(items)], refs[len(items) :]
    where = starts(place_ref)
    blocks = sorted({block for block, _ in items})
    pairs, need = [], {}
    for at, block in enumerate(blocks):
        need[block] = len(pairs)
        pairs.append((e_ref.at[pl.ds(where[block], ROWS), :], field.at[at]))
        for i, (its_block, pair) in enumerate(items):
            if its_block == block:
                for k in range(2):
                    need[i, k] = len(pairs)
                    pairs.append((panel_of(pieces[i], 2 * pair + k), held.at[2 * i + k]))
    pairs += list(zip(olds, [sums]))
    copies = fetch(pairs, sems)
    if first:
        sums[...] = jnp.zeros_like(sums)
    else:
        copies[-1].wait()
    for at, block in enumerate(blocks):
        copies[need[block]].wait()
        left = turned(field[at])
        for i, (its_block, pair) in enumerate(items):
            if its_block == block:
                for k in range(2):
                    copies[need[i, k]].wait()
                    sums[2 * pair + k] += crossed(left, *halves(held[2 * i + k]))
    if last:
        for k in range(4):
            out_ref[:, 8 * k : 8 * k + 8, :] = sums[k].T.reshape(32, 8, 128)
    else:
        end = pltpu.make_async_copy(sums, out_ref, sems.at[0])
        end.start()
        end.wait()


def hold_kernel(*refs):
    pieces, (out_ref, held, split, sems, out_sems) = refs[:16], refs[16:]
    slots = held.shape[0]

    def copies(block):
        slot = block % slots
        return [pltpu.make_async_copy(panel_of(pieces[2 * block + k // 2], k), held.at[slot, k], sems.at[slot, k]) for k in range(4)]

    def out(block):
        return pltpu.make_async_copy(split.at[block % 2], out_ref.at[block], out_sems.at[block % 2])

    for block in range(slots - 1):
        for copy in copies(block):
            copy.start()
    for block in range(8):
        if block + slots - 1 < 8:
            for copy in copies(block + slots - 1):
                copy.start()
        if block >= 2:
            out(block - 2).wait()
        for k, copy in enumerate(copies(block)):
            copy.wait()
            split[block % 2, k, 0], split[block % 2, k, 1] = halves(held[block % slots, k])
        out(block).start()
    out(6).wait()
    out(7).wait()


def last_kernel(place_ref, field_ref, factors_ref, sums_ref, mine_ref, other_ref, held_ref, out_ref,
                field, new, factors, sums, mine, other, held, sems, out_sems):
    where = starts(place_ref)
    pairs = [(sums_ref, sums), (factors_ref, factors), (mine_ref, mine), (other_ref, other)]
    for block in range(8):
        pairs += [(field_ref.at[pl.ds(where[block], ROWS), :], field.at[block]), (held_ref.at[block], held.at[block])]
    copies = fetch(pairs, sems)
    for copy in copies[:4]:
        copy.wait()

    def gram(k, j):
        half, at = divmod(BLOCKS.index((k, j)), 3)
        rows = pl.ds(256 * at, 256)
        return jnp.where(place_ref[1] == half, mine[rows, :], other[rows, :])

    coeffs = []
    for k in range(4):
        left = sums[:, 8 * k : 8 * k + 8, :].reshape(256, 128)
        for j in range(k):
            left = left - product(gram(k, j), coeffs[j])
        coeffs.append(product(factors[k], left))
    parts = []
    for high, low in map(halves, coeffs):
        parts.append((jnp.concatenate([high, low], axis=1), high))
    outs = []
    for block in range(8):
        copies[4 + 2 * block].wait()
        copies[5 + 2 * block].wait()
        total = None
        for k, (wide, high) in enumerate(parts):
            both = dot(held[block, k, 0], wide)
            part = both[:, :128] + both[:, 128:] + dot(held[block, k, 1], high)
            total = part if total is None else total + part
        new[block] = field[block] - total
        outs.append(pltpu.make_async_copy(new.at[block], out_ref.at[pl.ds(where[block], ROWS), :], out_sems.at[block]))
        outs[-1].start()
    for copy in outs:
        copy.wait()


def gram_kernel(place_ref, first_ref, second_ref, mine_ref, other_ref):
    panels = [first_ref[0], first_ref[1], second_ref[0], second_ref[1]]
    parts = [halves(panel) for panel in panels[:3]]
    for k in range(1, 4):
        lh, ll = halves(panels[k].T)
        for j in range(k):
            high, low = parts[j]
            block = dot(lh, high) + dot(lh, low) + dot(ll, high)
            half, at = divmod(BLOCKS.index((k, j)), 3)

            @pl.when(place_ref[1] == half)
            def _():
                mine_ref[256 * at : 256 * at + 256, :] = block

            @pl.when(place_ref[1] != half)
            def _():
                other_ref[256 * at : 256 * at + 256, :] = block


def spread_kernel(arrived_ref, out_ref):
    total = jnp.sum(arrived_ref[...], axis=0)
    out_ref[...] = jnp.broadcast_to(total[None], out_ref.shape)


def call(kernel, out, ins, outs, scratch, *args, limit=None):
    limit = limit or (60 if scratch else 16)
    return pl.pallas_call(kernel, out_shape=out, in_specs=ins, out_specs=outs, scratch_shapes=scratch,
                          compiler_params=pltpu.CompilerParams(vmem_limit_bytes=limit * 2**20))(*args)


def shifted(x, axis, step):
    size = lax.axis_size(axis)
    return lax.ppermute(x, axis, [(i, (i + step) % size) for i in range(size)])


def gathered(pair, own):
    behind = shifted(own, "x", 1)
    ahead = shifted(own, "x", -1)
    far = shifted(*((behind, "x", 1) if pair == 0 else (ahead, "x", -1)))
    mine = [behind, ahead, far]
    swapped = [shifted(part, "core", 1) for part in mine]
    return dict(zip((1, 2, 3, 5, 6, 7), mine + swapped))


def exchanged(tiles):
    return lax.all_to_all(tiles, ROW, split_axis=0, concat_axis=0, tiled=True)


def total(tiles):
    arrived = exchanged(tiles)
    copies = call(spread_kernel, jax.ShapeDtypeStruct(tiles.shape, F32), [VMEM], VMEM, [], arrived)
    return exchanged(copies)


def gram(pairs, place):
    share = jax.ShapeDtypeStruct((768, 256), F32)
    mine, other = call(gram_kernel, [share, share], [SMEM, VMEM, VMEM], [VMEM, VMEM], [], place, *pairs)
    mine = mine + shifted(other, "core", 1)
    part = exchanged(mine.reshape(32, 24, 256)).sum(axis=0)
    part = (part + shifted(part, "x", 2)) + (shifted(part, "x", 1) + shifted(part, "x", -1))
    copies = jnp.broadcast_to(lax.optimization_barrier(part), (32, 24, 256))
    mine = exchanged(copies).reshape(768, 256)
    return mine, shifted(mine, "core", 1)


def body(eigvecs, reflectors, factors):
    place = jnp.stack([lax.axis_index("x"), lax.axis_index("core")]).astype(jnp.int32)
    sem = pltpu.SemaphoreType.DMA
    own = [reflectors[:2], reflectors[2:]]
    swapped = shifted(reflectors, "core", 1)
    moving = [gathered(pair, own[pair]) for pair in range(2)]
    mine, other = gram(own, place)
    piece = lambda block, pair: {0: reflectors, 4: swapped}.get(block, moving[pair].get(block))
    everything = [piece(block, pair) for block in range(8) for pair in range(2)]

    def stage(items, olds, out, last=False):
        count = len({block for block, _ in items})
        return call(functools.partial(stage_kernel, items, not olds, last), out,
                    [SMEM, ANY] + [ANY] * (len(olds) + len(items)), VMEM if last else ANY,
                    [pltpu.VMEM((count, ROWS, 128), F32), pltpu.VMEM((2 * len(items), ROWS, 256), F32),
                     pltpu.VMEM((4, 128, 256), F32), sem((count + 2 * len(items) + 1,))],
                    place, eigvecs, *olds, *[piece(*item) for item in items])

    sums, tiles = jax.ShapeDtypeStruct((4, 128, 256), F32), jax.ShapeDtypeStruct((32, 32, 128), F32)
    state = stage(((0, 0), (0, 1), (4, 0), (4, 1)), [], sums)
    state = stage(((1, 0), (2, 1), (5, 0), (6, 1)), [state], sums)
    state = stage(((1, 1), (2, 0), (5, 1), (6, 0)), [state], sums)
    sums = total(stage(((3, 0), (3, 1), (7, 0), (7, 1)), [state], tiles, last=True))
    held = jax.ShapeDtypeStruct((8, 4, 2, ROWS, 256), BF16)
    held = call(hold_kernel, held, [ANY] * 16, ANY,
                [pltpu.VMEM((3, 4, ROWS, 256), F32), pltpu.VMEM((2, 4, 2, ROWS, 256), BF16), sem((3, 4)), sem((2,))], *everything)
    block = pltpu.VMEM((8, ROWS, 128), F32)
    share = pltpu.VMEM((768, 256), F32)
    return call(last_kernel, jax.ShapeDtypeStruct((4096, 128), F32), [SMEM] + [ANY] * 6, ANY,
                [block, block, pltpu.VMEM((4, 256, 256), F32), pltpu.VMEM((32, 32, 128), F32), share, share,
                 pltpu.VMEM((8, 4, 2, ROWS, 256), BF16), sem((20,)), sem((8,))],
                place, eigvecs, factors, sums, mine, other, held)


def solution(mesh):
    split = Mesh(mesh.devices.reshape(4, 8, 4, 2), (*ROW, *COL))
    in_specs = (P(ROW, COL), P(None, ROW + COL, None), P())
    return jax.shard_map(body, mesh=split, in_specs=in_specs, out_specs=P(ROW, COL), check_vma=False)
```

```python
import functools

import jax
import jax.numpy as jnp
from jax import lax
from jax.experimental import pallas as pl
from jax.experimental.pallas import tpu as pltpu
from jax.sharding import Mesh
from jax.sharding import PartitionSpec as P


ROW = ("y", "z")
COL = ("x", "core")
SMEM = pl.BlockSpec(memory_space=pltpu.SMEM)
VMEM = pl.BlockSpec(memory_space=pltpu.VMEM)
ANY = pl.BlockSpec(memory_space=pltpu.HBM)
F32, BF16 = jnp.float32, jnp.bfloat16
DISTANCES = (0, 3, 1, 2)
ROWS = 512
BLOCKS = ((1, 0), (2, 0), (2, 1), (3, 0), (3, 1), (3, 2))


def dot(left, right):
    return jnp.dot(left, right, preferred_element_type=F32)


def halves(x):
    high = x.astype(BF16)
    return high, (x - high.astype(F32)).astype(BF16)


def product(left, right):
    lh, ll = halves(left)
    rh, rl = halves(right)
    wide = dot(lh, jnp.concatenate([rh, rl], axis=1))
    return wide[:, :128] + wide[:, 128:] + dot(ll, rh)


def starts(place_ref):
    out = []
    for side in range(2):
        for distance in DISTANCES:
            block = lax.rem(place_ref[0] + distance, 4) * 2 + lax.rem(place_ref[1] + side, 2)
            out.append(pl.multiple_of(block * ROWS, ROWS))
    return out


def fetch(pairs, sems):
    copies = [pltpu.make_async_copy(source, target, sems.at[i]) for i, (source, target) in enumerate(pairs)]
    for copy in copies:
        copy.start()
    return copies


def panel_of(piece, panel):
    return piece.at[panel if piece.shape[0] == 4 else panel % 2]


def turned(x):
    high, low = halves(x.T)
    return jnp.concatenate([high, low], axis=0)


def crossed(left, high, low):
    wide = dot(left, high)
    return wide[:128] + wide[128:] + dot(left[:128], low)


def stage_kernel(items, first, last, place_ref, e_ref, *refs):
    olds, refs = (refs[:0], refs) if first else (refs[:1], refs[1:])
    pieces, (out_ref, field, held, sums, sems) = refs[: len(items)], refs[len(items) :]
    where = starts(place_ref)
    blocks = sorted({block for block, _ in items})
    pairs, need = [], {}
    for at, block in enumerate(blocks):
        need[block] = len(pairs)
        pairs.append((e_ref.at[pl.ds(where[block], ROWS), :], field.at[at]))
        for i, (its_block, pair) in enumerate(items):
            if its_block == block:
                for k in range(2):
                    need[i, k] = len(pairs)
                    pairs.append((panel_of(pieces[i], 2 * pair + k), held.at[2 * i + k]))
    pairs += list(zip(olds, [sums]))
    copies = fetch(pairs, sems)
    if first:
        sums[...] = jnp.zeros_like(sums)
    else:
        copies[-1].wait()
    for at, block in enumerate(blocks):
        copies[need[block]].wait()
        left = turned(field[at])
        for i, (its_block, pair) in enumerate(items):
            if its_block == block:
                for k in range(2):
                    copies[need[i, k]].wait()
                    sums[2 * pair + k] += crossed(left, *halves(held[2 * i + k]))
    if last:
        for k in range(4):
            out_ref[:, 8 * k : 8 * k + 8, :] = sums[k].T.reshape(32, 8, 128)
    else:
        end = pltpu.make_async_copy(sums, out_ref, sems.at[0])
        end.start()
        end.wait()


def hold_kernel(*refs):
    pieces, (out_ref, held, split, sems, out_sems) = refs[:16], refs[16:]
    slots = held.shape[0]

    def copies(block):
        slot = block % slots
        return [pltpu.make_async_copy(panel_of(pieces[2 * block + k // 2], k), held.at[slot, k], sems.at[slot, k]) for k in range(4)]

    def out(block):
        return pltpu.make_async_copy(split.at[block % 2], out_ref.at[block], out_sems.at[block % 2])

    for block in range(slots - 1):
        for copy in copies(block):
            copy.start()
    for block in range(8):
        if block + slots - 1 < 8:
            for copy in copies(block + slots - 1):
                copy.start()
        if block >= 2:
            out(block - 2).wait()
        for k, copy in enumerate(copies(block)):
            copy.wait()
            split[block % 2, k, 0], split[block % 2, k, 1] = halves(held[block % slots, k])
        out(block).start()
    out(6).wait()
    out(7).wait()


def last_kernel(place_ref, field_ref, factors_ref, sums, mine_ref, other_ref, held_ref, out_ref,
                field, new, factors, mine, other, held, sems, out_sems):
    where = starts(place_ref)
    pairs = [(factors_ref, factors), (mine_ref, mine), (other_ref, other)]
    for block in range(8):
        pairs += [(field_ref.at[pl.ds(where[block], ROWS), :], field.at[block]), (held_ref.at[block], held.at[block])]
    copies = fetch(pairs, sems)
    for copy in copies[:3]:
        copy.wait()

    def gram(k, j):
        half, at = divmod(BLOCKS.index((k, j)), 3)
        rows = pl.ds(256 * at, 256)
        return jnp.where(place_ref[1] == half, mine[rows, :], other[rows, :])

    lefts, parts = [sums[:, 8 * k : 8 * k + 8, :].reshape(256, 128) for k in range(4)], []
    for k in range(4):
        for i in range(k + 1, 4):
            lefts[i] = lefts[i] - product(gram(i, k), lefts[k])
        high, low = halves(product(factors[k], lefts[k]))
        parts.append((jnp.concatenate([high, low], axis=1), high))
    outs = []
    for block in range(8):
        copies[3 + 2 * block].wait()
        copies[4 + 2 * block].wait()
        total = None
        for k, (wide, high) in enumerate(parts):
            both = dot(held[block, k, 0], wide)
            part = both[:, :128] + both[:, 128:] + dot(held[block, k, 1], high)
            total = part if total is None else total + part
        new[block] = field[block] - total
        outs.append(pltpu.make_async_copy(new.at[block], out_ref.at[pl.ds(where[block], ROWS), :], out_sems.at[block]))
        outs[-1].start()
    for copy in outs:
        copy.wait()


def gram_kernel(place_ref, first_ref, second_ref, factors_ref, mine_ref, other_ref):
    panels = [first_ref[0], first_ref[1], second_ref[0], second_ref[1]]
    scaled = []
    for j in range(3):
        vh, vl = halves(panels[j])
        th, tl = halves(factors_ref[j])
        scaled.append(halves(dot(vh, th) + dot(vh, tl) + dot(vl, th)))
    for k in range(1, 4):
        lh, ll = halves(panels[k].T)
        for j in range(k):
            high, low = scaled[j]
            block = dot(lh, high) + dot(lh, low) + dot(ll, high)
            half, at = divmod(BLOCKS.index((k, j)), 3)

            @pl.when(place_ref[1] == half)
            def _():
                mine_ref[256 * at : 256 * at + 256, :] = block

            @pl.when(place_ref[1] != half)
            def _():
                other_ref[256 * at : 256 * at + 256, :] = block


def spread_kernel(arrived_ref, out_ref):
    total = jnp.sum(arrived_ref[...], axis=0)
    out_ref[...] = jnp.broadcast_to(total[None], out_ref.shape)


def call(kernel, out, ins, outs, scratch, *args, limit=None):
    limit = limit or (60 if scratch else 16)
    return pl.pallas_call(kernel, out_shape=out, in_specs=ins, out_specs=outs, scratch_shapes=scratch,
                          compiler_params=pltpu.CompilerParams(vmem_limit_bytes=limit * 2**20))(*args)


def shifted(x, axis, step):
    size = lax.axis_size(axis)
    return lax.ppermute(x, axis, [(i, (i + step) % size) for i in range(size)])


def gathered(pair, own):
    behind = shifted(own, "x", 1)
    ahead = shifted(own, "x", -1)
    far = shifted(*((behind, "x", 1) if pair == 0 else (ahead, "x", -1)))
    mine = [behind, ahead, far]
    swapped = [shifted(part, "core", 1) for part in mine]
    return dict(zip((1, 2, 3, 5, 6, 7), mine + swapped))


def exchanged(tiles):
    return lax.all_to_all(tiles, ROW, split_axis=0, concat_axis=0, tiled=True)


def total(tiles):
    arrived = exchanged(tiles)
    copies = call(spread_kernel, jax.ShapeDtypeStruct(tiles.shape, F32), [VMEM], VMEM, [], arrived)
    return exchanged(copies)


def gram(pairs, factors, place):
    share = jax.ShapeDtypeStruct((768, 256), F32)
    mine, other = call(gram_kernel, [share, share], [SMEM] + [VMEM] * 3, [VMEM, VMEM], [], place, *pairs, factors)
    mine = mine + shifted(other, "core", 1)
    part = exchanged(mine.reshape(32, 24, 256)).sum(axis=0)
    part = (part + shifted(part, "x", 2)) + (shifted(part, "x", 1) + shifted(part, "x", -1))
    copies = jnp.broadcast_to(lax.optimization_barrier(part), (32, 24, 256))
    mine = exchanged(copies).reshape(768, 256)
    return mine, shifted(mine, "core", 1)


def body(eigvecs, reflectors, factors):
    place = jnp.stack([lax.axis_index("x"), lax.axis_index("core")]).astype(jnp.int32)
    sem = pltpu.SemaphoreType.DMA
    own = [reflectors[:2], reflectors[2:]]
    swapped = shifted(reflectors, "core", 1)
    moving = [gathered(pair, own[pair]) for pair in range(2)]
    mine, other = gram(own, factors, place)
    piece = lambda block, pair: {0: reflectors, 4: swapped}.get(block, moving[pair].get(block))
    everything = [piece(block, pair) for block in range(8) for pair in range(2)]

    def stage(items, olds, out, last=False):
        count = len({block for block, _ in items})
        return call(functools.partial(stage_kernel, items, not olds, last), out,
                    [SMEM, ANY] + [ANY] * (len(olds) + len(items)), VMEM if last else ANY,
                    [pltpu.VMEM((count, ROWS, 128), F32), pltpu.VMEM((2 * len(items), ROWS, 256), F32),
                     pltpu.VMEM((4, 128, 256), F32), sem((count + 2 * len(items) + 1,))],
                    place, eigvecs, *olds, *[piece(*item) for item in items], limit=24 if last else None)

    sums, tiles = jax.ShapeDtypeStruct((4, 128, 256), F32), jax.ShapeDtypeStruct((32, 32, 128), F32)
    state = stage(((0, 0), (0, 1), (4, 0), (4, 1)), [], sums)
    state = stage(((1, 0), (2, 1), (5, 0), (6, 1)), [state], sums)
    state = stage(((1, 1), (2, 0), (5, 1), (6, 0)), [state], sums)
    sums = total(stage(((3, 0), (3, 1), (7, 0), (7, 1)), [state], tiles, last=True))
    held = jax.ShapeDtypeStruct((8, 4, 2, ROWS, 256), BF16)
    held = call(hold_kernel, held, [ANY] * 16, ANY,
                [pltpu.VMEM((3, 4, ROWS, 256), F32), pltpu.VMEM((2, 4, 2, ROWS, 256), BF16), sem((3, 4)), sem((2,))], *everything)
    block = pltpu.VMEM((8, ROWS, 128), F32)
    share = pltpu.VMEM((768, 256), F32)
    return call(last_kernel, jax.ShapeDtypeStruct((4096, 128), F32), [SMEM, ANY, ANY, VMEM, ANY, ANY, ANY], ANY,
                [block, block, pltpu.VMEM((4, 256, 256), F32), share, share,
                 pltpu.VMEM((8, 4, 2, ROWS, 256), BF16), sem((19,)), sem((8,))],
                place, eigvecs, factors, sums, mine, other, held)


def solution(mesh):
    split = Mesh(mesh.devices.reshape(4, 8, 4, 2), (*ROW, *COL))
    in_specs = (P(ROW, COL), P(None, ROW + COL, None), P())
    return jax.shard_map(body, mesh=split, in_specs=in_specs, out_specs=P(ROW, COL), check_vma=False)
```
